16 devices in a mesh: data: 4 (over z, y), time: 4 (over x, core).
Axes of the slice: x: 2, y: 2, z: 2, core: 2. Of those that a mesh axis runs over, the one named last changes fastest.
Arguments:
- x_init: float32 [128, 16, 256], P('data'), parts along dimension 0
- w_in: bfloat16 [256, 1024], replicated
- w_out: bfloat16 [1024, 256], replicated
- mod_gamma: bfloat16 [32, 1024], P('time')
- mod_beta: bfloat16 [32, 1024], P('time')
- step_size: float32 [32], P('time')
Outputs:
- output: float32 [128, 16, 256], P('data'), parts along dimension 0
There are 4 independent parts. The reference program is written for one: setup_inputs(seed, part) draws one part's arguments, and reference() takes and returns one part's arrays. A program takes and returns all parts, laid end to end along the dimension named above; an argument that names none is the same for every part.
All inputs are finite; a program needn't handle non-finite values.
Results may differ from the reference program's by a relative error of at most 0.00135424.
Values are sent between devices in bfloat16 or wider.
A program may use at most 1 GiB of HBM per device.

```python
import jax
import jax.numpy as jnp
from jax import lax

SAMPLES = 32
TOKENS = 16
CHANNELS = 256
HIDDEN = 1024
NUM_STEPS = 32
SWEEPS = 4


def setup_inputs(seed: int = 0, part: int = 0) -> dict:
    base_key = jax.random.key(seed)
    part_key = jax.random.fold_in(base_key, part)
    sub_keys = jax.random.split(base_key, 6)
    x_init = jax.random.normal(part_key, (SAMPLES, TOKENS, CHANNELS), jnp.float32)
    w_in = (jax.random.normal(sub_keys[0], (CHANNELS, HIDDEN), jnp.float32) * CHANNELS ** -0.5).astype(jnp.bfloat16)
    w_out = (jax.random.normal(sub_keys[1], (HIDDEN, CHANNELS), jnp.float32) * HIDDEN ** -0.5).astype(jnp.bfloat16)
    mod_gamma = (0.5 * jax.random.normal(sub_keys[2], (NUM_STEPS, HIDDEN), jnp.float32)).astype(jnp.bfloat16)
    mod_beta = jax.random.normal(sub_keys[3], (NUM_STEPS, HIDDEN), jnp.float32).astype(jnp.bfloat16)
    total_time = 1.0 + 2.0 * jax.random.uniform(sub_keys[4], (), jnp.float32)
    step_size = (0.5 + jax.random.uniform(sub_keys[5], (NUM_STEPS,), jnp.float32)) * (total_time / NUM_STEPS)
    return {"x_init": x_init, "w_in": w_in, "w_out": w_out, "mod_gamma": mod_gamma, "mod_beta": mod_beta, "step_size": step_size}


def drift_of(latents, w_in, w_out, gamma_j, beta_j, h_step):
    pre_act = jnp.dot(latents.astype(jnp.bfloat16).reshape(-1, CHANNELS), w_in, preferred_element_type=jnp.float32)
    hidden_act = jax.nn.gelu(pre_act * (1.0 + gamma_j.astype(jnp.float32)) + beta_j.astype(jnp.float32), approximate=True).astype(jnp.bfloat16)
    proj_out = jnp.dot(hidden_act, w_out, preferred_element_type=jnp.float32)
    return h_step * proj_out.reshape(latents.shape)


def reference(x_init, w_in, w_out, mod_gamma, mod_beta, step_size):
    run_init = jnp.zeros((SWEEPS,) + x_init.shape, jnp.float32)

    def step_body(run_sums, step_in):
        gamma_j, beta_j, h_step = step_in
        latents = jnp.concatenate([x_init[None], x_init[None] + run_sums[:-1]], axis=0)
        return run_sums + drift_of(latents, w_in, w_out, gamma_j, beta_j, h_step), None

    run_sums, _ = lax.scan(step_body, run_init, (mod_gamma, mod_beta, step_size))
    return x_init + run_sums[-1]
```

```python
import functools

import jax
import jax.numpy as jnp
from jax import lax
from jax.experimental import pallas as pl
from jax.experimental.pallas import tpu as pltpu
from jax.sharding import PartitionSpec as P

SWEEPS = 4
STEPS = 32
ROWS = 128
C = 256
H = 1024
TILE = 256
TILES = H // TILE
FIRST = [0, 32, 63, 93, 122]
U0 = 4
U1 = 5
BLOCK = 16
PIECES = 4
GELU_C = 0.7978845608028654
F32 = jnp.float32
BF16 = jnp.bfloat16
MESH = pl.DeviceIdType.MESH


def step_of(unit):
    unit = jnp.int32(unit)
    sweep = (unit >= FIRST[1]).astype(jnp.int32) + (unit >= FIRST[2]).astype(jnp.int32) + (unit >= FIRST[3]).astype(jnp.int32)
    return unit - jnp.where(sweep == 0, 0, jnp.where(sweep == 1, FIRST[1] - 1, jnp.where(sweep == 2, FIRST[2] - 2, FIRST[3] - 3)))


def kernel(h_ref, x_hbm, w_in_hbm, w_out_hbm, gamma_ref, beta_ref, y_hbm,
           w_in, w_out, gamma_raw, beta_raw, h_raw, gain, shift, hidden0, pre, act, latent, drift,
           load_sem, mod_send, mod_recv, out_sem, near_send, near_recv, far_send, far_recv, pass_send, pass_recv):
    me = lax.axis_index("time")
    group = lax.axis_index("data")
    near = me + 1 - 2 * lax.rem(me, 2)
    far = lax.rem(me + 2, 4)
    diag = lax.rem(near + 2, 4)
    peers = (near, far, diag)

    def rows_of(device):
        return pl.ds(pl.multiple_of(device * ROWS, ROWS), ROWS)

    loads = [pltpu.make_async_copy(x_hbm.at[rows_of(me)], latent.at[FIRST[1] - 1], load_sem.at[0])]
    for n in range(TILES):
        loads.append(pltpu.make_async_copy(w_in_hbm.at[:, pl.ds(n * TILE, TILE)], w_in.at[n], load_sem.at[1 + n]))
    loads.append(pltpu.make_async_copy(w_out_hbm, w_out, load_sem.at[1 + TILES]))
    for load in loads:
        load.start()

    barrier = pltpu.get_barrier_semaphore()
    for peer in peers:
        pl.semaphore_signal(barrier, inc=1, device_id=(group, peer), device_id_type=MESH)
    for k in range(8):
        h_raw[me, pl.ds(k, 1), :] = jnp.full((1, 128), h_ref[k], F32)
    gamma_raw[me] = gamma_ref[...]
    beta_raw[me] = beta_ref[...]
    pl.semaphore_wait(barrier, 3)

    sends = []
    for p, peer in enumerate(peers):
        for a, (src, dst) in enumerate(((gamma_ref, gamma_raw), (beta_ref, beta_raw), (h_raw.at[me], h_raw))):
            send = pltpu.make_async_remote_copy(
                src_ref=src, dst_ref=dst.at[me], send_sem=mod_send.at[p, a], recv_sem=mod_recv.at[me, a],
                device_id=(group, peer), device_id_type=MESH)
            send.start()
            sends.append(send)

    def dot(a, b):
        return lax.dot_general(a, b, (((1,), (0,)), ((), ())), precision=lax.Precision.DEFAULT, preferred_element_type=F32)

    for load in loads[:-1]:
        load.wait()
    x_own = latent[FIRST[1] - 1]
    for n in range(TILES):
        hidden0[:, n * TILE:(n + 1) * TILE] = dot(x_own, w_in[n])

    for peer in peers:
        for a, dst in enumerate((gamma_raw, beta_raw, h_raw)):
            pltpu.make_async_remote_copy(
                src_ref=dst.at[peer], dst_ref=dst.at[peer], send_sem=mod_send.at[0, a], recv_sem=mod_recv.at[peer, a],
                device_id=(group, peer), device_id_type=MESH).wait_recv()
    for d in range(4):
        gain[pl.ds(d * 8, 8), :] = 0.5 + 0.5 * gamma_raw[d].astype(F32)
        shift[pl.ds(d * 8, 8), :] = 0.5 * beta_raw[d].astype(F32)
    loads[-1].wait()

    def activate(src, base, n, units, shared):
        cols = slice(n * TILE, (n + 1) * TILE)
        for k in range(units):
            j = step_of(base + k)
            a = jnp.broadcast_to(gain[pl.ds(j, 1), cols], (BLOCK, TILE))
            b = jnp.broadcast_to(shift[pl.ds(j, 1), cols], (BLOCK, TILE))
            for r in range(0, ROWS, BLOCK):
                q = r if shared else k * ROWS + r
                half = src[q:q + BLOCK, cols] * a + b
                u = half * ((8 * GELU_C * 0.044715) * (half * half) + 2 * GELU_C)
                act[k * ROWS + r:k * ROWS + r + BLOCK, cols] = half * jnp.tanh(u) + half

    def project_out(units):
        drift[0:units * ROWS] = dot(act[0:units * ROWS, :], w_out[...])

    def project_in(base, units, n):
        rows = latent[pl.ds(base, units)].reshape(units * ROWS, C)
        pre[0:units * ROWS, n * TILE:(n + 1) * TILE] = dot(rows, w_in[n])

    def accumulate(base, units):
        for k in range(units):
            unit = jnp.int32(base + k)
            h = jnp.broadcast_to(h_raw[step_of(unit) // 8, pl.ds(lax.rem(step_of(unit), 8), 1), :], (ROWS, 128))
            first = (unit == FIRST[1]) | (unit == FIRST[2]) | (unit == FIRST[3])
            ahead = jnp.where(unit < FIRST[1], 32, jnp.where(unit < FIRST[2], 31, 30))
            start = jnp.where(first, unit, unit + ahead - 1)
            for c in range(0, C, 128):
                latent[unit + ahead, :, c:c + 128] = latent[start, :, c:c + 128] + drift[k * ROWS:(k + 1) * ROWS, c:c + 128] * h

    for n in range(TILES):
        activate(hidden0, 0, n, U0, True)

    def sweep0(t, carry):
        project_out(U0)
        for n in range(TILES):
            activate(hidden0, t * U0, n, U0, True)
        accumulate((t - 1) * U0, U0)
        return carry

    lax.fori_loop(1, STEPS // U0, sweep0, 0)
    project_out(U0)
    accumulate(STEPS - U0, U0)
    for n in range(TILES):
        project_in(FIRST[1], U1, n)
    for n in range(TILES):
        activate(pre, FIRST[1], n, U1, False)
        project_in(FIRST[1] + U1, U1, n)

    count = (FIRST[4] - FIRST[1]) // U1

    def later(t, carry):
        base = FIRST[1] + t * U1
        project_out(U1)
        for n in range(TILES):
            activate(pre, base + U1, n, U1, False)
            project_in(base + 2 * U1, U1, n)
        accumulate(base, U1)
        return carry

    lax.fori_loop(0, count - 2, later, 0)
    project_out(U1)
    for n in range(TILES):
        activate(pre, FIRST[4] - U1, n, U1, False)
    accumulate(FIRST[4] - 2 * U1, U1)
    project_out(U1)
    accumulate(FIRST[4] - U1, U1)

    y_own = latent.at[FIRST[4] - 1 + 30]
    piece = ROWS // PIECES

    def part(device, k):
        return pl.ds(pl.multiple_of(device * ROWS + k * piece, piece), piece)

    far_copies = []
    for k in range(PIECES):
        copy = pltpu.make_async_remote_copy(
            src_ref=y_own.at[pl.ds(k * piece, piece)], dst_ref=y_hbm.at[part(me, k)], send_sem=far_send.at[k],
            recv_sem=far_recv.at[k], device_id=(group, far), device_id_type=MESH)
        copy.start()
        far_copies.append(copy)
    near_copy = pltpu.make_async_remote_copy(
        src_ref=y_own, dst_ref=y_hbm.at[rows_of(me)], send_sem=near_send, recv_sem=near_recv,
        device_id=(group, near), device_id_type=MESH)
    near_copy.start()
    own_copy = pltpu.make_async_copy(y_own, y_hbm.at[rows_of(me)], out_sem)
    own_copy.start()
    pass_copies = []
    for k in range(PIECES):
        far_copies[k].wait_recv()
        copy = pltpu.make_async_remote_copy(
            src_ref=y_hbm.at[part(far, k)], dst_ref=y_hbm.at[part(far, k)], send_sem=pass_send.at[k],
            recv_sem=pass_recv.at[k], device_id=(group, near), device_id_type=MESH)
        copy.start()
        pass_copies.append(copy)
    near_copy.wait_recv()
    for copy in pass_copies:
        copy.wait_recv()
    own_copy.wait()
    near_copy.wait_send()
    for copy in far_copies + pass_copies + sends:
        copy.wait_send()


def solution(mesh):
    vmem = pltpu.VMEM
    units = max(U0, U1)

    def local_run(x_init, w_in, w_out, mod_gamma, mod_beta, step_size):
        hbm = pl.BlockSpec(memory_space=pl.ANY)
        out = pl.pallas_call(
            kernel,
            out_shape=jax.ShapeDtypeStruct((4 * ROWS, C), F32),
            in_specs=[pl.BlockSpec(memory_space=pltpu.SMEM), hbm, hbm, hbm, pl.BlockSpec(memory_space=vmem), pl.BlockSpec(memory_space=vmem)],
            out_specs=hbm,
            scratch_shapes=[
                vmem((TILES, C, TILE), BF16), vmem((H, C), BF16),
                vmem((4, 8, H), BF16), vmem((4, 8, H), BF16), vmem((4, 8, 128), F32),
                vmem((STEPS, H), F32), vmem((STEPS, H), F32),
                vmem((ROWS, H), F32), vmem((units * ROWS, H), F32), vmem((units * ROWS, H), F32),
                vmem((FIRST[4] + 32, ROWS, C), F32), vmem((units * ROWS, C), F32),
                pltpu.SemaphoreType.DMA((2 + TILES,)),
                pltpu.SemaphoreType.DMA((3, 3)), pltpu.SemaphoreType.DMA((4, 3)),
                pltpu.SemaphoreType.DMA, pltpu.SemaphoreType.DMA, pltpu.SemaphoreType.DMA,
                pltpu.SemaphoreType.DMA((PIECES,)), pltpu.SemaphoreType.DMA((PIECES,)),
                pltpu.SemaphoreType.DMA((PIECES,)), pltpu.SemaphoreType.DMA((PIECES,)),
            ],
            compiler_params=pltpu.CompilerParams(collective_id=0, has_side_effects=True, vmem_limit_bytes=60 * 2 ** 20),
            name="picard",
        )(step_size, x_init.reshape(4 * ROWS, C), w_in, w_out, mod_gamma, mod_beta)
        return out.reshape(x_init.shape)

    return jax.shard_map(local_run, mesh=mesh, in_specs=(P("data", None, None), P(None, None), P(None, None), P("time", None), P("time", None), P("time")), out_specs=P("data", None, None), check_vma=False)
```

```python
import jax
import jax.numpy as jnp
from jax import lax
from jax.experimental import pallas as pl
from jax.experimental.pallas import tpu as pltpu
from jax.sharding import PartitionSpec as P

STEPS = 32
OWN = 8
ROWS = 128
C = 256
H = 1024
TILE = 256
TILES = H // TILE
FIRST = [0, 32, 63, 93, 122]
UNITS = 6
TAIL = 18
SECTION = 32
SECTIONS = ROWS // SECTION
CHUNKS = (FIRST[4] - TAIL - FIRST[1]) // UNITS
BATCH = UNITS * ROWS
TAIL_BATCH = TAIL * SECTION
STRIP = 16
GELU_C = 0.7978845608028654
F32 = jnp.float32
BF16 = jnp.bfloat16
MESH = pl.DeviceIdType.MESH


def span(first, count):
    return slice(first, first + count) if isinstance(first, int) else pl.ds(first, count)


def sweep_values(unit, values):
    if isinstance(unit, int):
        return values[0] if unit < FIRST[2] else values[1] if unit < FIRST[3] else values[2]
    return jnp.where(unit < FIRST[2], values[0], jnp.where(unit < FIRST[3], values[1], values[2]))


def step_of(unit):
    return unit - sweep_values(unit, (FIRST[1] - 1, FIRST[2] - 2, FIRST[3] - 3))


def kernel(h_hbm, x_hbm, w_in_hbm, w_out_hbm, gamma_hbm, beta_hbm, y,
           w_in, w_out, gamma_raw, beta_raw, h_own, h_rows, gain, shift, hidden0, pre, act, latent, drift, drift0,
           load_sem, mod_send, mod_recv, near_send, near_recv, far_send, far_recv, pass_send, pass_recv):
    me = lax.axis_index("time")
    group = lax.axis_index("data")
    core = lax.rem(me, 2)
    near = me + 1 - 2 * core
    far = lax.rem(me + 2, 4)
    diag = lax.rem(near + 2, 4)
    peers = (near, far, diag)

    def rows_of(device, first=0, count=ROWS):
        return pl.ds(pl.multiple_of(device * ROWS + first, 8), count)

    def steps_of(device):
        return pl.ds(pl.multiple_of(device * OWN, OWN), OWN)

    loads = [
        pltpu.make_async_copy(gamma_hbm, gamma_raw.at[me], load_sem.at[0]),
        pltpu.make_async_copy(beta_hbm, beta_raw.at[me], load_sem.at[1]),
        pltpu.make_async_copy(h_hbm, h_own, load_sem.at[2]),
        pltpu.make_async_copy(x_hbm.at[rows_of(me)], latent.at[FIRST[1] - 1], load_sem.at[3]),
    ]
    for n in range(TILES):
        loads.append(pltpu.make_async_copy(w_in_hbm.at[:, pl.ds(n * TILE, TILE)], w_in.at[n], load_sem.at[4 + n]))
    loads.append(pltpu.make_async_copy(w_out_hbm, w_out, load_sem.at[4 + TILES]))
    for load in loads:
        load.start()

    barrier = pltpu.get_barrier_semaphore()
    for peer in peers:
        pl.semaphore_signal(barrier, inc=1, device_id=(group, peer), device_id_type=MESH)
    for load in loads[:3]:
        load.wait()
    for k in range(OWN):
        h_rows[pl.ds(me * OWN + k, 1), :] = jnp.broadcast_to(h_own[:, k:k + 1], (1, 128))
    pl.semaphore_wait(barrier, 3)

    def mod_copy(p, peer, source):
        refs = (gamma_raw.at[source], beta_raw.at[source], h_rows.at[steps_of(source)])
        return [
            pltpu.make_async_remote_copy(
                src_ref=ref, dst_ref=ref, send_sem=mod_send.at[p, a], recv_sem=mod_recv.at[source, a],
                device_id=(group, peer), device_id_type=MESH)
            for a, ref in enumerate(refs)
        ]

    sends = []
    for p, peer in enumerate(peers):
        sends += mod_copy(p, peer, me)
    for send in sends:
        send.start()

    def dot(a, b):
        return lax.dot_general(a, b, (((1,), (0,)), ((), ())), precision=lax.Precision.DEFAULT, preferred_element_type=F32)

    def modulation(device):
        gain[steps_of(device), :] = 0.5 + 0.5 * gamma_raw[device].astype(F32)
        shift[steps_of(device), :] = 0.5 * beta_raw[device].astype(F32)

    def gelu(pre_act, a, b):
        half = pre_act * a + b
        u = half * ((8 * GELU_C * 0.044715) * (half * half) + 2 * GELU_C)
        return half * jnp.tanh(u) + half

    def activate(source, n, count, rows, mod, shared=False):
        cols = slice(n * TILE, (n + 1) * TILE)
        for k in range(count):
            a, b = mod(k, cols)
            for r in range(0, rows, STRIP):
                q = r if shared else k * rows + r
                act[k * rows + r:k * rows + r + STRIP, cols] = gelu(source[q:q + STRIP, cols], a, b)

    def mod_rows(steps):
        def rows(k, cols):
            row = span(steps[k], 1)
            return jnp.broadcast_to(gain[row, cols], (STRIP, TILE)), jnp.broadcast_to(shift[row, cols], (STRIP, TILE))
        return rows

    for load in loads[3:-1]:
        load.wait()
    modulation(me)
    x_own = latent[FIRST[1] - 1]
    for n in range(TILES):
        hidden0[:, n * TILE:(n + 1) * TILE] = dot(x_own, w_in[n])

    def steps0(device):
        return mod_rows([device * OWN + k for k in range(OWN)])

    def project0(device):
        half = OWN * ROWS // 2
        for i in range(2):
            rows = pl.ds(pl.multiple_of(device * (OWN * ROWS) + i * half, half), half)
            drift0[rows] = dot(act[i * half:(i + 1) * half, :], w_out[...])

    def chain0(first, last):
        for r in range(0, ROWS, 64):
            for c in range(0, C, 128):
                total = latent[FIRST[1] - 1 + first, r:r + 64, c:c + 128]
                for j in range(first, last):
                    h = jnp.broadcast_to(h_rows[j:j + 1, :], (64, 128))
                    total = total + drift0[j * ROWS + r:j * ROWS + r + 64, c:c + 128] * h
                    latent[FIRST[1] + j, r:r + 64, c:c + 128] = total

    other = 2 - 2 * (me // 2)

    def ordered(k):
        if isinstance(k, int):
            return (me, near, other, other + 1)[k]
        return jnp.where(k == 0, me, jnp.where(k == 1, near, other + k - 2))

    for n in range(TILES):
        activate(hidden0, n, OWN, ROWS, steps0(me), True)
    loads[-1].wait()

    def loop0(k, carry):
        for copy in mod_copy(0, near, ordered(k)):
            copy.wait_recv()
        modulation(ordered(k))
        project0(ordered(k - 1))
        for n in range(TILES):
            activate(hidden0, n, OWN, ROWS, steps0(ordered(k)), True)
        return carry

    lax.fori_loop(1, 4, loop0, 0)

    def chunk(t):
        return FIRST[1] + t * UNITS

    def unit_mods(base):
        return mod_rows([step_of(base + k) for k in range(UNITS)])

    def project_in(base, n):
        rows = latent[span(base, UNITS)].reshape(BATCH, C)
        pre[:, n * TILE:(n + 1) * TILE] = dot(rows, w_in[n])

    def project_out(count, parts=1):
        rows = count // parts
        return [dot(act[i * rows:(i + 1) * rows, :], w_out[...]) for i in range(parts)]

    def keep(drifts):
        first = 0
        for part in drifts:
            drift[first:first + part.shape[0]] = part
            first += part.shape[0]

    def accumulate(base, idle=None):
        for k in range(UNITS):
            unit = base + k
            if idle is not None:
                unit = jnp.where(idle, FIRST[4] - 1, unit)
            h = jnp.broadcast_to(h_rows[span(step_of(unit), 1), :], (ROWS, 128))
            ahead = sweep_values(unit, (31, 30, 30))
            if isinstance(unit, int):
                start = unit if unit in FIRST else unit + ahead - 1
            else:
                start = jnp.where((unit == FIRST[1]) | (unit == FIRST[2]) | (unit == FIRST[3]), unit, unit + ahead - 1)
            for c in range(0, C, 128):
                latent[unit + ahead, :, c:c + 128] = latent[start, :, c:c + 128] + drift[k * ROWS:(k + 1) * ROWS, c:c + 128] * h

    parity = []

    def step(body):
        parity.append(0)
        pl.when(me < 4 if len(parity) % 2 else me >= 0)(body)

    chain0(0, OWN)

    @step
    def _():
        for n in range(TILES):
            project_in(chunk(0), n)
        project0(ordered(3))
        for n in range(TILES):
            activate(pre, n, UNITS, ROWS, unit_mods(chunk(0)))

    @step
    def _():
        chain0(OWN, 2 * OWN)
        for n in range(TILES - 1):
            project_in(chunk(1), n)
        chain0(2 * OWN, STEPS)

    def loop(t, carry):
        base = chunk(t)
        project_in(base + UNITS, TILES - 1)
        drifts = project_out(BATCH)
        for n in range(TILES):
            activate(pre, n, UNITS, ROWS, unit_mods(base + UNITS))
            if n < TILES - 1:
                project_in(base + 2 * UNITS, n)
        accumulate(base - UNITS, t == 0)
        keep(drifts)
        return carry

    lax.fori_loop(0, CHUNKS - 2, loop, 0)

    tail = mod_rows(list(range(STEPS - TAIL, STEPS)))

    def section_in(q, n):
        rows = latent[FIRST[4] - TAIL:FIRST[4], q * SECTION:(q + 1) * SECTION].reshape(TAIL_BATCH, C)
        pre[0:TAIL_BATCH, n * TILE:(n + 1) * TILE] = dot(rows, w_in[n])

    def finish(q):
        for c in range(0, C, 128):
            total = latent[FIRST[4] - TAIL - 1 + 30, q * SECTION:(q + 1) * SECTION, c:c + 128]
            for k in range(TAIL):
                h = jnp.broadcast_to(h_rows[STEPS - TAIL + k:STEPS - TAIL + k + 1, :], (SECTION, 128))
                total = total + drift[k * SECTION:(k + 1) * SECTION, c:c + 128] * h
            y[rows_of(me, q * SECTION, SECTION), c:c + 128] = total

    def section_copy(q, source, target, send, recv):
        ref = y.at[rows_of(source, q * SECTION, SECTION)]
        return pltpu.make_async_remote_copy(
            src_ref=ref, dst_ref=ref, send_sem=send.at[q], recv_sem=recv.at[q], device_id=(group, target), device_id_type=MESH)

    def section_copies(q):
        return [section_copy(q, me, far, far_send, far_recv), section_copy(q, me, near, near_send, near_recv)]

    def send_section(q):
        for copy in section_copies(q):
            copy.start()

    def into(t, n):
        if t < CHUNKS:
            project_in(chunk(t), n)
        elif t < CHUNKS + SECTIONS:
            section_in(t - CHUNKS, n)

    def through(t, n):
        if t < CHUNKS:
            activate(pre, n, UNITS, ROWS, unit_mods(chunk(t)))
        elif t < CHUNKS + SECTIONS:
            activate(pre, n, TAIL, SECTION, tail)

    def tail_step(t):
        def body():
            into(t + 1, TILES - 1)
            if t <= CHUNKS:
                accumulate(chunk(t - 1))
            drifts = project_out(BATCH if t < CHUNKS else TAIL_BATCH)
            for n in range(TILES):
                through(t + 1, n)
                if n < TILES - 1:
                    into(t + 2, n)
            keep(drifts)
        return body

    for t in range(CHUNKS - 2, CHUNKS + SECTIONS - 1):
        if t > CHUNKS:
            step(lambda: finish(t - 1 - CHUNKS))
            send_section(t - 1 - CHUNKS)
        step(tail_step(t))
    step(lambda: finish(SECTIONS - 2))
    send_section(SECTIONS - 2)

    @step
    def _():
        keep(project_out(TAIL_BATCH, 2))
        finish(SECTIONS - 1)

    send_section(SECTIONS - 1)

    own_copies = [section_copies(q) for q in range(SECTIONS)]
    pass_copies = [section_copy(q, far, near, pass_send, pass_recv) for q in range(SECTIONS)]
    for (far_copy, _), pass_copy in zip(own_copies, pass_copies):
        far_copy.wait_recv()
        pass_copy.start()
    for (_, near_copy), pass_copy in zip(own_copies, pass_copies):
        near_copy.wait_recv()
        pass_copy.wait_recv()
    for copy in sends + [copy for copies in own_copies for copy in copies] + pass_copies:
        copy.wait_send()


def solution(mesh):
    vmem = pltpu.VMEM
    dma = pltpu.SemaphoreType.DMA
    sections = dma((SECTIONS,))
    def local_run(x_init, w_in, w_out, mod_gamma, mod_beta, step_size):
        hbm = pl.BlockSpec(memory_space=pl.ANY)
        out = pl.pallas_call(
            kernel,
            out_shape=vmem((4 * ROWS, C), F32),
            in_specs=[hbm] * 6,
            out_specs=pl.BlockSpec(memory_space=vmem),
            scratch_shapes=[
                vmem((TILES, C, TILE), BF16), vmem((H, C), BF16),
                vmem((4, OWN, H), BF16), vmem((4, OWN, H), BF16), vmem((1, OWN), F32), vmem((STEPS, 128), F32),
                vmem((STEPS, H), F32), vmem((STEPS, H), F32),
                vmem((ROWS, H), F32), vmem((BATCH, H), F32), vmem((OWN * ROWS, H), F32),
                vmem((FIRST[4] + 32, ROWS, C), F32), vmem((BATCH, C), F32), vmem((STEPS * ROWS, C), F32),
                dma((5 + TILES,)), dma((3, 3)), dma((4, 3)),
                sections, sections, sections, sections, sections, sections,
            ],
            compiler_params=pltpu.CompilerParams(collective_id=0, has_side_effects=True, vmem_limit_bytes=60 * 2 ** 20),
            name="picard",
        )(step_size.reshape(1, OWN), x_init.reshape(4 * ROWS, C), w_in, w_out, mod_gamma, mod_beta)
        return out.reshape(x_init.shape)

    return jax.shard_map(local_run, mesh=mesh, in_specs=(P("data", None, None), P(None, None), P(None, None), P("time", None), P("time", None), P("time")), out_specs=P("data", None, None), check_vma=False)
```

```python
import jax
import jax.numpy as jnp
from jax import lax
from jax.experimental import pallas as pl
from jax.experimental.pallas import tpu as pltpu
from jax.sharding import PartitionSpec as P

STEPS = 32
OWN = 8
ROWS = 128
C = 256
H = 1024
TILE = 256
TILES = H // TILE
FIRST = [0, 32, 63, 93, 122]
UNITS = 6
TAIL = 18
SECTION = 32
SECTIONS = ROWS // SECTION
CHUNKS = (FIRST[4] - TAIL - FIRST[1]) // UNITS
BATCH = UNITS * ROWS
TAIL_BATCH = TAIL * SECTION
STRIP = 16
GELU_C = 0.7978845608028654
F32 = jnp.float32
BF16 = jnp.bfloat16
MESH = pl.DeviceIdType.MESH


def span(first, count):
    return slice(first, first + count) if isinstance(first, int) else pl.ds(first, count)


def sweep_values(unit, values):
    if isinstance(unit, int):
        return values[0] if unit < FIRST[2] else values[1] if unit < FIRST[3] else values[2]
    return jnp.where(unit < FIRST[2], values[0], jnp.where(unit < FIRST[3], values[1], values[2]))


def step_of(unit):
    return unit - sweep_values(unit, (FIRST[1] - 1, FIRST[2] - 2, FIRST[3] - 3))


def kernel(h_hbm, x_hbm, w_in_hbm, w_out_hbm, gamma_hbm, beta_hbm, y,
           w_in, w_out, gamma_raw, beta_raw, h_own, h_rows, gain, shift, hidden0, pre, act, latent, drift, drift0,
           load_sem, mod_send, mod_recv, near_send, near_recv, far_send, far_recv, pass_send, pass_recv):
    me = lax.axis_index("time")
    group = lax.axis_index("data")
    core = lax.rem(me, 2)
    near = me + 1 - 2 * core
    far = lax.rem(me + 2, 4)
    diag = lax.rem(near + 2, 4)
    peers = (near, far, diag)

    def rows_of(device, first=0, count=ROWS):
        return pl.ds(pl.multiple_of(device * ROWS + first, 8), count)

    def steps_of(device):
        return pl.ds(pl.multiple_of(device * OWN, OWN), OWN)

    loads = [
        pltpu.make_async_copy(gamma_hbm, gamma_raw.at[me], load_sem.at[0]),
        pltpu.make_async_copy(beta_hbm, beta_raw.at[me], load_sem.at[1]),
        pltpu.make_async_copy(h_hbm, h_own, load_sem.at[2]),
        pltpu.make_async_copy(x_hbm.at[rows_of(me)], latent.at[FIRST[1] - 1], load_sem.at[3]),
    ]
    for n in range(TILES):
        loads.append(pltpu.make_async_copy(w_in_hbm.at[:, pl.ds(n * TILE, TILE)], w_in.at[n], load_sem.at[4 + n]))
    loads.append(pltpu.make_async_copy(w_out_hbm, w_out, load_sem.at[4 + TILES]))
    for load in loads:
        load.start()

    barrier = pltpu.get_barrier_semaphore()
    for peer in peers:
        pl.semaphore_signal(barrier, inc=1, device_id=(group, peer), device_id_type=MESH)
    for load in loads[:2]:
        load.wait()
    pl.semaphore_wait(barrier, 3)

    def mod_copy(p, peer, source):
        refs = (gamma_raw.at[source], beta_raw.at[source], h_rows.at[steps_of(source)])
        return [
            pltpu.make_async_remote_copy(
                src_ref=ref, dst_ref=ref, send_sem=mod_send.at[p, a], recv_sem=mod_recv.at[source, a],
                device_id=(group, peer), device_id_type=MESH)
            for a, ref in enumerate(refs)
        ]

    sends = []
    for p, peer in enumerate(peers):
        sends += mod_copy(p, peer, me)
    for a, send in enumerate(sends):
        if a % 3 < 2:
            send.start()

    def dot(a, b):
        return lax.dot_general(a, b, (((1,), (0,)), ((), ())), precision=lax.Precision.DEFAULT, preferred_element_type=F32)

    def modulation(device):
        gain[steps_of(device), :] = 0.5 + 0.5 * gamma_raw[device].astype(F32)
        shift[steps_of(device), :] = 0.5 * beta_raw[device].astype(F32)

    def gelu(pre_act, a, b):
        half = pre_act * a + b
        u = half * ((8 * GELU_C * 0.044715) * (half * half) + 2 * GELU_C)
        return half * jnp.tanh(u) + half

    def activate(source, n, count, rows, mod, shared=False):
        cols = slice(n * TILE, (n + 1) * TILE)
        for k in range(count):
            a, b = mod(k, cols)
            for r in range(0, rows, STRIP):
                q = r if shared else k * rows + r
                act[k * rows + r:k * rows + r + STRIP, cols] = gelu(source[q:q + STRIP, cols], a, b)

    def mod_rows(steps):
        def rows(k, cols):
            row = span(steps[k], 1)
            return jnp.broadcast_to(gain[row, cols], (STRIP, TILE)), jnp.broadcast_to(shift[row, cols], (STRIP, TILE))
        return rows

    for load in loads[2:-1]:
        load.wait()
    modulation(me)
    for k in range(OWN):
        h_rows[pl.ds(me * OWN + k, 1), :] = jnp.broadcast_to(h_own[:, k:k + 1], (1, 128))
    x_own = latent[FIRST[1] - 1]
    for n in range(TILES):
        hidden0[:, n * TILE:(n + 1) * TILE] = dot(x_own, w_in[n])

    def steps0(device):
        return mod_rows([device * OWN + k for k in range(OWN)])

    def project0(device):
        half = OWN * ROWS // 2
        for i in range(2):
            rows = pl.ds(pl.multiple_of(device * (OWN * ROWS) + i * half, half), half)
            drift0[rows] = dot(act[i * half:(i + 1) * half, :], w_out[...])

    def chain0(first, last):
        for r in range(0, ROWS, 64):
            for c in range(0, C, 128):
                total = latent[FIRST[1] - 1 + first, r:r + 64, c:c + 128]
                for j in range(first, last):
                    h = jnp.broadcast_to(h_rows[j:j + 1, :], (64, 128))
                    total = total + drift0[j * ROWS + r:j * ROWS + r + 64, c:c + 128] * h
                    latent[FIRST[1] + j, r:r + 64, c:c + 128] = total

    other = 2 - 2 * (me // 2)

    def ordered(k):
        if isinstance(k, int):
            return (me, near, other, other + 1)[k]
        return jnp.where(k == 0, me, jnp.where(k == 1, near, other + k - 2))

    for n in range(TILES):
        activate(hidden0, n, OWN, ROWS, steps0(me), True)
    for send in sends[2::3]:
        send.start()
    loads[-1].wait()

    def loop0(k, carry):
        for copy in mod_copy(0, near, ordered(k))[:2]:
            copy.wait_recv()
        modulation(ordered(k))
        project0(ordered(k - 1))
        for n in range(TILES):
            activate(hidden0, n, OWN, ROWS, steps0(ordered(k)), True)
        return carry

    lax.fori_loop(1, 4, loop0, 0)
    for k in range(1, 4):
        mod_copy(0, near, ordered(k))[2].wait_recv()

    def chunk(t):
        return FIRST[1] + t * UNITS

    def unit_mods(base):
        return mod_rows([step_of(base + k) for k in range(UNITS)])

    def project_in(base, n):
        rows = latent[span(base, UNITS)].reshape(BATCH, C)
        pre[:, n * TILE:(n + 1) * TILE] = dot(rows, w_in[n])

    def project_out(count, parts=1):
        rows = count // parts
        return [dot(act[i * rows:(i + 1) * rows, :], w_out[...]) for i in range(parts)]

    def keep(drifts):
        first = 0
        for part in drifts:
            drift[first:first + part.shape[0]] = part
            first += part.shape[0]

    def accumulate(base, idle=None):
        for k in range(UNITS):
            unit = base + k
            if idle is not None:
                unit = jnp.where(idle, FIRST[4] - 1, unit)
            h = jnp.broadcast_to(h_rows[span(step_of(unit), 1), :], (ROWS, 128))
            ahead = sweep_values(unit, (31, 30, 30))
            if isinstance(unit, int):
                start = unit if unit in FIRST else unit + ahead - 1
            else:
                start = jnp.where((unit == FIRST[1]) | (unit == FIRST[2]) | (unit == FIRST[3]), unit, unit + ahead - 1)
            for c in range(0, C, 128):
                latent[unit + ahead, :, c:c + 128] = latent[start, :, c:c + 128] + drift[k * ROWS:(k + 1) * ROWS, c:c + 128] * h

    def steps(*bodies):
        def turn(i, carry):
            for k, body in enumerate(bodies):
                pl.when(i == k)(body)
            return carry

        lax.fori_loop(0, len(bodies), turn, 0)

    chain0(0, OWN)

    def first_chunk():
        for n in range(TILES):
            project_in(chunk(0), n)
        project0(ordered(3))
        for n in range(TILES):
            activate(pre, n, UNITS, ROWS, unit_mods(chunk(0)))

    def second_chunk():
        chain0(OWN, 2 * OWN)
        for n in range(TILES - 1):
            project_in(chunk(1), n)
        chain0(2 * OWN, STEPS)

    steps(first_chunk, second_chunk)

    def loop(t, carry):
        base = chunk(t)
        project_in(base + UNITS, TILES - 1)
        drifts = project_out(BATCH)
        for n in range(TILES):
            activate(pre, n, UNITS, ROWS, unit_mods(base + UNITS))
            if n < TILES - 1:
                project_in(base + 2 * UNITS, n)
        accumulate(base - UNITS, t == 0)
        keep(drifts)
        return carry

    lax.fori_loop(0, CHUNKS - 2, loop, 0)

    tail = mod_rows(list(range(STEPS - TAIL, STEPS)))

    def section_in(q, n):
        rows = latent[FIRST[4] - TAIL:FIRST[4], q * SECTION:(q + 1) * SECTION].reshape(TAIL_BATCH, C)
        pre[0:TAIL_BATCH, n * TILE:(n + 1) * TILE] = dot(rows, w_in[n])

    def finish(q):
        for c in range(0, C, 128):
            total = latent[FIRST[4] - TAIL - 1 + 30, q * SECTION:(q + 1) * SECTION, c:c + 128]
            for k in range(TAIL):
                h = jnp.broadcast_to(h_rows[STEPS - TAIL + k:STEPS - TAIL + k + 1, :], (SECTION, 128))
                total = total + drift[k * SECTION:(k + 1) * SECTION, c:c + 128] * h
            y[rows_of(me, q * SECTION, SECTION), c:c + 128] = total

    def section_copy(q, source, target, send, recv):
        ref = y.at[rows_of(source, q * SECTION, SECTION)]
        return pltpu.make_async_remote_copy(
            src_ref=ref, dst_ref=ref, send_sem=send.at[q], recv_sem=recv.at[q], device_id=(group, target), device_id_type=MESH)

    def section_copies(q):
        copies = [section_copy(q, me, far, far_send, far_recv), section_copy(q, me, near, near_send, near_recv)]
        if q == SECTIONS - 1:
            copies.append(section_copy(q, me, diag, pass_send, pass_recv))
        return copies

    def send_section(q):
        for copy in section_copies(q):
            copy.start()

    def into(t, n):
        if t < CHUNKS:
            project_in(chunk(t), n)
        elif t < CHUNKS + SECTIONS:
            section_in(t - CHUNKS, n)

    def through(t, n):
        if t < CHUNKS:
            activate(pre, n, UNITS, ROWS, unit_mods(chunk(t)))
        elif t < CHUNKS + SECTIONS:
            activate(pre, n, TAIL, SECTION, tail)

    def tail_step(t):
        def body():
            if t > CHUNKS:
                finish(t - 1 - CHUNKS)
                send_section(t - 1 - CHUNKS)
            if t + 1 == CHUNKS + SECTIONS:
                keep(project_out(TAIL_BATCH, 2))
                finish(SECTIONS - 1)
                return
            into(t + 1, TILES - 1)
            if t <= CHUNKS:
                accumulate(chunk(t - 1))
            drifts = project_out(BATCH if t < CHUNKS else TAIL_BATCH)
            for n in range(TILES):
                through(t + 1, n)
                if n < TILES - 1:
                    into(t + 2, n)
            keep(drifts)
        return body

    steps(tail_step(CHUNKS - 2), tail_step(CHUNKS - 1))
    steps(tail_step(CHUNKS), tail_step(CHUNKS + 1))
    steps(tail_step(CHUNKS + 2), tail_step(CHUNKS + 3))
    send_section(SECTIONS - 1)

    own_copies = [section_copies(q) for q in range(SECTIONS)]
    pass_copies = [section_copy(q, far, near, pass_send, pass_recv) for q in range(SECTIONS - 1)]
    for q, copies in enumerate(own_copies):
        copies[0].wait_recv()
        if q < SECTIONS - 1:
            pass_copies[q].start()
    for q, copies in enumerate(own_copies):
        copies[1].wait_recv()
        (pass_copies[q] if q < SECTIONS - 1 else copies[2]).wait_recv()
    for copy in sends + [copy for copies in own_copies for copy in copies] + pass_copies:
        copy.wait_send()


def solution(mesh):
    vmem = pltpu.VMEM
    dma = pltpu.SemaphoreType.DMA
    sections = dma((SECTIONS,))
    def local_run(x_init, w_in, w_out, mod_gamma, mod_beta, step_size):
        hbm = pl.BlockSpec(memory_space=pl.ANY)
        out = pl.pallas_call(
            kernel,
            out_shape=vmem((4 * ROWS, C), F32),
            in_specs=[hbm] * 6,
            out_specs=pl.BlockSpec(memory_space=vmem),
            scratch_shapes=[
                vmem((TILES, C, TILE), BF16), vmem((H, C), BF16),
                vmem((4, OWN, H), BF16), vmem((4, OWN, H), BF16), vmem((1, OWN), F32), vmem((STEPS, 128), F32),
                vmem((STEPS, H), F32), vmem((STEPS, H), F32),
                vmem((ROWS, H), F32), vmem((BATCH, H), F32), vmem((OWN * ROWS, H), F32),
                vmem((FIRST[4] + 32, ROWS, C), F32), vmem((BATCH, C), F32), vmem((STEPS * ROWS, C), F32),
                dma((5 + TILES,)), dma((3, 3)), dma((4, 3)),
                sections, sections, sections, sections, sections, sections,
            ],
            compiler_params=pltpu.CompilerParams(collective_id=0, has_side_effects=True, vmem_limit_bytes=60 * 2 ** 20),
            name="picard",
        )(step_size.reshape(1, OWN), x_init.reshape(4 * ROWS, C), w_in, w_out, mod_gamma, mod_beta)
        return out.reshape(x_init.shape)

    return jax.shard_map(local_run, mesh=mesh, in_specs=(P("data", None, None), P(None, None), P(None, None), P("time", None), P("time", None), P("time")), out_specs=P("data", None, None), check_vma=False)
```

```python
import jax
import jax.numpy as jnp
from jax import lax
from jax.experimental import pallas as pl
from jax.experimental.pallas import tpu as pltpu
from jax.sharding import PartitionSpec as P

STEPS = 32
OWN = 8
ROWS = 128
C = 256
H = 1024
TILE = 256
TILES = H // TILE
FIRST = [0, 32, 63, 93, 122]
UNITS = 6
TAIL = 18
SECTION = 32
SECTIONS = ROWS // SECTION
CHUNKS = (FIRST[4] - TAIL - FIRST[1]) // UNITS
BATCH = UNITS * ROWS
TAIL_BATCH = TAIL * SECTION
EARLY = (FIRST[3] - 2 - FIRST[1]) // UNITS >= CHUNKS - 2
STRIP = 16
GELU_C = 0.7978845608028654
F32 = jnp.float32
BF16 = jnp.bfloat16
MESH = pl.DeviceIdType.MESH


def span(first, count):
    return slice(first, first + count) if isinstance(first, int) else pl.ds(first, count)


def sweep_values(unit, values):
    if isinstance(unit, int):
        return values[0] if unit < FIRST[2] else values[1] if unit < FIRST[3] else values[2]
    return jnp.where(unit < FIRST[2], values[0], jnp.where(unit < FIRST[3], values[1], values[2]))


def step_of(unit):
    return unit - sweep_values(unit, (FIRST[1] - 1, FIRST[2] - 2, FIRST[3] - 3))


def kernel(h_hbm, x_hbm, w_in_hbm, w_out_hbm, gamma_hbm, beta_hbm, y,
           w_in, w_out, gamma_raw, beta_raw, h_own, h_rows, gain, shift, hidden0, pre, act, latent, drift, drift0,
           load_sem, mod_send, mod_recv, near_send, near_recv, far_send, far_recv, pass_send, pass_recv):
    me = lax.axis_index("time")
    group = lax.axis_index("data")
    core = lax.rem(me, 2)
    near = me + 1 - 2 * core
    far = lax.rem(me + 2, 4)
    diag = lax.rem(near + 2, 4)
    peers = (near, far, diag)

    def rows_of(device, first=0, count=ROWS):
        return pl.ds(pl.multiple_of(device * ROWS + first, 8), count)

    def steps_of(device):
        return pl.ds(pl.multiple_of(device * OWN, OWN), OWN)

    loads = [
        pltpu.make_async_copy(gamma_hbm, gamma_raw.at[me], load_sem.at[0]),
        pltpu.make_async_copy(beta_hbm, beta_raw.at[me], load_sem.at[1]),
        pltpu.make_async_copy(h_hbm, h_own, load_sem.at[2]),
        pltpu.make_async_copy(x_hbm.at[rows_of(me)], latent.at[FIRST[1] - 1], load_sem.at[3]),
    ]
    for n in range(TILES):
        loads.append(pltpu.make_async_copy(w_in_hbm.at[:, pl.ds(n * TILE, TILE)], w_in.at[n], load_sem.at[4 + n]))
    loads.append(pltpu.make_async_copy(w_out_hbm, w_out, load_sem.at[4 + TILES]))
    for load in loads:
        load.start()

    barrier = pltpu.get_barrier_semaphore()
    for peer in peers:
        pl.semaphore_signal(barrier, inc=1, device_id=(group, peer), device_id_type=MESH)
    for load in loads[:2]:
        load.wait()
    pl.semaphore_wait(barrier, 3)

    def mod_copy(p, peer, source):
        refs = (gamma_raw.at[source], beta_raw.at[source], h_rows.at[steps_of(source)])
        return [
            pltpu.make_async_remote_copy(
                src_ref=ref, dst_ref=ref, send_sem=mod_send.at[p, a], recv_sem=mod_recv.at[source, a],
                device_id=(group, peer), device_id_type=MESH)
            for a, ref in enumerate(refs)
        ]

    sends = []
    for p, peer in enumerate(peers):
        sends += mod_copy(p, peer, me)
    for a, send in enumerate(sends):
        if a % 3 < 2:
            send.start()

    def dot(a, b):
        return lax.dot_general(a, b, (((1,), (0,)), ((), ())), precision=lax.Precision.DEFAULT, preferred_element_type=F32)

    def modulation(device):
        gain[steps_of(device), :] = 0.5 + 0.5 * gamma_raw[device].astype(F32)
        shift[steps_of(device), :] = 0.5 * beta_raw[device].astype(F32)

    def gelu(pre_act, a, b):
        half = pre_act * a + b
        u = half * ((8 * GELU_C * 0.044715) * (half * half) + 2 * GELU_C)
        return half * jnp.tanh(u) + half

    def activate(source, n, count, rows, mod, shared=False):
        cols = slice(n * TILE, (n + 1) * TILE)
        for k in range(count):
            a, b = mod(k, cols)
            for r in range(0, rows, STRIP):
                q = r if shared else k * rows + r
                act[k * rows + r:k * rows + r + STRIP, cols] = gelu(source[q:q + STRIP, cols], a, b)

    def mod_rows(steps):
        def rows(k, cols):
            row = span(steps[k], 1)
            return jnp.broadcast_to(gain[row, cols], (STRIP, TILE)), jnp.broadcast_to(shift[row, cols], (STRIP, TILE))
        return rows

    for load in loads[2:-1]:
        load.wait()
    modulation(me)
    for k in range(OWN):
        h_rows[pl.ds(me * OWN + k, 1), :] = jnp.broadcast_to(h_own[:, k:k + 1], (1, 128))
    x_own = latent[FIRST[1] - 1]
    for n in range(TILES):
        hidden0[:, n * TILE:(n + 1) * TILE] = dot(x_own, w_in[n])

    def steps0(device):
        return mod_rows([device * OWN + k for k in range(OWN)])

    def project0(device):
        half = OWN * ROWS // 2
        for i in range(2):
            rows = pl.ds(pl.multiple_of(device * (OWN * ROWS) + i * half, half), half)
            drift0[rows] = dot(act[i * half:(i + 1) * half, :], w_out[...])

    def chain0(first, last):
        for r in range(0, ROWS, 64):
            for c in range(0, C, 128):
                total = latent[FIRST[1] - 1 + first, r:r + 64, c:c + 128]
                for j in range(first, last):
                    h = jnp.broadcast_to(h_rows[j:j + 1, :], (64, 128))
                    total = total + drift0[j * ROWS + r:j * ROWS + r + 64, c:c + 128] * h
                    latent[FIRST[1] + j, r:r + 64, c:c + 128] = total

    other = 2 - 2 * (me // 2)

    def ordered(k):
        if isinstance(k, int):
            return (me, near, other, other + 1)[k]
        return jnp.where(k == 0, me, jnp.where(k == 1, near, other + k - 2))

    for n in range(TILES):
        activate(hidden0, n, OWN, ROWS, steps0(me), True)
    for send in sends[2::3]:
        send.start()
    loads[-1].wait()

    def loop0(k, carry):
        for copy in mod_copy(0, near, ordered(k))[:2]:
            copy.wait_recv()
        modulation(ordered(k))
        project0(ordered(k - 1))
        for n in range(TILES):
            activate(hidden0, n, OWN, ROWS, steps0(ordered(k)), True)
        return carry

    lax.fori_loop(1, 4, loop0, 0)
    for k in range(1, 4):
        mod_copy(0, near, ordered(k))[2].wait_recv()

    def chunk(t):
        return FIRST[1] + t * UNITS

    def unit_mods(base):
        return mod_rows([step_of(base + k) for k in range(UNITS)])

    def project_in(base, n):
        rows = latent[span(base, UNITS)].reshape(BATCH, C)
        pre[:, n * TILE:(n + 1) * TILE] = dot(rows, w_in[n])

    def project_out(count, parts=1):
        rows = count // parts
        return [dot(act[i * rows:(i + 1) * rows, :], w_out[...]) for i in range(parts)]

    def keep(drifts):
        first = 0
        for part in drifts:
            drift[first:first + part.shape[0]] = part
            first += part.shape[0]

    def accumulate(base):
        for k in range(UNITS):
            unit = base + k
            h = jnp.broadcast_to(h_rows[span(step_of(unit), 1), :], (ROWS, 128))
            ahead = sweep_values(unit, (31, 30, 30))
            if isinstance(unit, int):
                start = unit if unit in FIRST else unit + ahead - 1
            else:
                start = jnp.where((unit == FIRST[1]) | (unit == FIRST[2]) | (unit == FIRST[3]), unit, unit + ahead - 1)
            for c in range(0, C, 128):
                latent[unit + ahead, :, c:c + 128] = latent[start, :, c:c + 128] + drift[k * ROWS:(k + 1) * ROWS, c:c + 128] * h

    def steps(*bodies):
        def turn(i, carry):
            for k, body in enumerate(bodies):
                pl.when(i == k)(body)
            return carry

        lax.fori_loop(0, len(bodies), turn, 0)

    chain0(0, OWN)

    def first_chunk():
        for n in range(TILES):
            project_in(chunk(0), n)
        project0(ordered(3))
        for n in range(TILES):
            activate(pre, n, UNITS, ROWS, unit_mods(chunk(0)))

    def second_chunk():
        chain0(OWN, 2 * OWN)
        for n in range(TILES - 1):
            project_in(chunk(1), n)
        chain0(2 * OWN, STEPS)

    steps(first_chunk, second_chunk)

    def loop(t, carry):
        base = chunk(t)
        project_in(base + UNITS, TILES - 1)
        drifts = project_out(BATCH)
        for n in range(TILES):
            activate(pre, n, UNITS, ROWS, unit_mods(base + UNITS))
            if n < TILES - 1:
                project_in(base + 2 * UNITS, n)
        keep(drifts)
        accumulate(base)
        return carry

    lax.fori_loop(0, CHUNKS - 2, loop, 0)

    tail = mod_rows(list(range(STEPS - TAIL, STEPS)))

    def section_in(q, n):
        rows = latent[FIRST[4] - TAIL:FIRST[4], q * SECTION:(q + 1) * SECTION].reshape(TAIL_BATCH, C)
        pre[0:TAIL_BATCH, n * TILE:(n + 1) * TILE] = dot(rows, w_in[n])

    def finish(q):
        for c in range(0, C, 128):
            total = latent[FIRST[4] - TAIL - 1 + 30, q * SECTION:(q + 1) * SECTION, c:c + 128]
            for k in range(TAIL):
                h = jnp.broadcast_to(h_rows[STEPS - TAIL + k:STEPS - TAIL + k + 1, :], (SECTION, 128))
                total = total + drift[k * SECTION:(k + 1) * SECTION, c:c + 128] * h
            y[rows_of(me, q * SECTION, SECTION), c:c + 128] = total

    def section_copy(q, source, target, send, recv):
        ref = y.at[rows_of(source, q * SECTION, SECTION)]
        return pltpu.make_async_remote_copy(
            src_ref=ref, dst_ref=ref, send_sem=send.at[q], recv_sem=recv.at[q], device_id=(group, target), device_id_type=MESH)

    def section_copies(q):
        copies = [section_copy(q, me, far, far_send, far_recv), section_copy(q, me, near, near_send, near_recv)]
        if q == SECTIONS - 1:
            copies.append(section_copy(q, me, diag, pass_send, pass_recv))
        return copies

    def send_section(q):
        for copy in section_copies(q):
            copy.start()

    def into(t, n):
        if t < CHUNKS:
            project_in(chunk(t), n)
        elif t < CHUNKS + SECTIONS:
            section_in(t - CHUNKS, n)

    def through(t, n):
        if t < CHUNKS:
            activate(pre, n, UNITS, ROWS, unit_mods(chunk(t)))
        elif t < CHUNKS + SECTIONS:
            activate(pre, n, TAIL, SECTION, tail)

    def tail_step(t):
        def body():
            into(t + 1, TILES - 1)
            drifts = project_out(BATCH if t < CHUNKS else TAIL_BATCH, 2 if EARLY and t == CHUNKS - 2 else 1)
            if EARLY and t == CHUNKS - 2:
                keep(drifts)
                accumulate(chunk(t))
            for n in range(TILES):
                through(t + 1, n)
                if n < TILES - 1:
                    into(t + 2, n)
            if not (EARLY and t == CHUNKS - 2):
                keep(drifts)
                if t < CHUNKS:
                    accumulate(chunk(t))
            if t >= CHUNKS:
                finish(t - CHUNKS)
                send_section(t - CHUNKS)
        return body

    def before_last():
        into(CHUNKS + SECTIONS - 1, TILES - 1)
        drifts = project_out(TAIL_BATCH, 2)
        for n in range(2):
            through(CHUNKS + SECTIONS - 1, n)
        keep(drifts)
        finish(SECTIONS - 2)
        send_section(SECTIONS - 2)

    def last():
        for n in range(2, TILES):
            through(CHUNKS + SECTIONS - 1, n)
        keep(project_out(TAIL_BATCH, 2))
        finish(SECTIONS - 1)

    steps(tail_step(CHUNKS - 2), tail_step(CHUNKS - 1))
    steps(tail_step(CHUNKS), tail_step(CHUNKS + 1))
    steps(before_last, last)
    send_section(SECTIONS - 1)

    own_copies = [section_copies(q) for q in range(SECTIONS)]
    pass_copies = [section_copy(q, far, near, pass_send, pass_recv) for q in range(SECTIONS - 1)]
    for q, copies in enumerate(own_copies):
        copies[0].wait_recv()
        if q < SECTIONS - 1:
            pass_copies[q].start()
    for q, copies in enumerate(own_copies):
        copies[1].wait_recv()
        (pass_copies[q] if q < SECTIONS - 1 else copies[2]).wait_recv()
    for copy in sends + [copy for copies in own_copies for copy in copies] + pass_copies:
        copy.wait_send()


def solution(mesh):
    vmem = pltpu.VMEM
    dma = pltpu.SemaphoreType.DMA
    sections = dma((SECTIONS,))
    def local_run(x_init, w_in, w_out, mod_gamma, mod_beta, step_size):
        hbm = pl.BlockSpec(memory_space=pl.ANY)
        out = pl.pallas_call(
            kernel,
            out_shape=vmem((4 * ROWS, C), F32),
            in_specs=[hbm] * 6,
            out_specs=pl.BlockSpec(memory_space=vmem),
            scratch_shapes=[
                vmem((TILES, C, TILE), BF16), vmem((H, C), BF16),
                vmem((4, OWN, H), BF16), vmem((4, OWN, H), BF16), vmem((1, OWN), F32), vmem((STEPS, 128), F32),
                vmem((STEPS, H), F32), vmem((STEPS, H), F32),
                vmem((ROWS, H), F32), vmem((BATCH, H), F32), vmem((OWN * ROWS, H), F32),
                vmem((FIRST[4] + 32, ROWS, C), F32), vmem((BATCH, C), F32), vmem((STEPS * ROWS, C), F32),
                dma((5 + TILES,)), dma((3, 3)), dma((4, 3)),
                sections, sections, sections, sections, sections, sections,
            ],
            compiler_params=pltpu.CompilerParams(collective_id=0, has_side_effects=True, vmem_limit_bytes=60 * 2 ** 20),
            name="picard",
        )(step_size.reshape(1, OWN), x_init.reshape(4 * ROWS, C), w_in, w_out, mod_gamma, mod_beta)
        return out.reshape(x_init.shape)

    return jax.shard_map(local_run, mesh=mesh, in_specs=(P("data", None, None), P(None, None), P(None, None), P("time", None), P("time", None), P("time")), out_specs=P("data", None, None), check_vma=False)
```

```python
import jax
import jax.numpy as jnp
from jax import lax
from jax.experimental import pallas as pl
from jax.experimental.pallas import tpu as pltpu
from jax.sharding import PartitionSpec as P

STEPS = 32
OWN = 8
ROWS = 128
C = 256
H = 1024
TILE = 256
TILES = H // TILE
FIRST = [0, 32, 63, 93, 122]
UNITS = 6
TAIL = 18
SECTION = 32
SECTIONS = ROWS // SECTION
CHUNKS = (FIRST[4] - TAIL - FIRST[1]) // UNITS
BATCH = UNITS * ROWS
TAIL_BATCH = TAIL * SECTION
EARLY = (FIRST[3] - 2 - FIRST[1]) // UNITS >= CHUNKS - 2
STRIP = 16
GELU_C = 0.7978845608028654
F32 = jnp.float32
BF16 = jnp.bfloat16
MESH = pl.DeviceIdType.MESH


def span(first, count):
    return slice(first, first + count) if isinstance(first, int) else pl.ds(first, count)


def sweep_values(unit, values):
    if isinstance(unit, int):
        return values[0] if unit < FIRST[2] else values[1] if unit < FIRST[3] else values[2]
    return jnp.where(unit < FIRST[2], values[0], jnp.where(unit < FIRST[3], values[1], values[2]))


def step_of(unit):
    return unit - sweep_values(unit, (FIRST[1] - 1, FIRST[2] - 2, FIRST[3] - 3))


def kernel(h_hbm, x_hbm, w_in_hbm, w_out_hbm, gamma_hbm, beta_hbm, y,
           w_in, w_out, gamma_raw, beta_raw, h_own, h_rows, gain, shift, hidden0, pre, act, latent, drift, drift0,
           load_sem, mod_send, mod_recv, near_send, near_recv, far_send, far_recv, pass_send, pass_recv):
    me = lax.axis_index("time")
    group = lax.axis_index("data")
    core = lax.rem(me, 2)
    near = me + 1 - 2 * core
    far = lax.rem(me + 2, 4)
    diag = lax.rem(near + 2, 4)
    peers = (near, far, diag)

    def rows_of(device, first=0, count=ROWS):
        return pl.ds(pl.multiple_of(device * ROWS + first, 8), count)

    def steps_of(device):
        return pl.ds(pl.multiple_of(device * OWN, OWN), OWN)

    loads = [
        pltpu.make_async_copy(gamma_hbm, gamma_raw.at[me], load_sem.at[0]),
        pltpu.make_async_copy(beta_hbm, beta_raw.at[me], load_sem.at[1]),
        pltpu.make_async_copy(h_hbm, h_own, load_sem.at[2]),
        pltpu.make_async_copy(x_hbm.at[rows_of(me)], latent.at[FIRST[1] - 1], load_sem.at[3]),
    ]
    for n in range(TILES):
        loads.append(pltpu.make_async_copy(w_in_hbm.at[:, pl.ds(n * TILE, TILE)], w_in.at[n], load_sem.at[4 + n]))
    loads.append(pltpu.make_async_copy(w_out_hbm, w_out, load_sem.at[4 + TILES]))
    for load in loads:
        load.start()

    barrier = pltpu.get_barrier_semaphore()
    for peer in peers:
        pl.semaphore_signal(barrier, inc=1, device_id=(group, peer), device_id_type=MESH)
    for load in loads[:2]:
        load.wait()
    pl.semaphore_wait(barrier, 3)

    def mod_copy(p, peer, source):
        refs = (gamma_raw.at[source], beta_raw.at[source], h_rows.at[steps_of(source)])
        return [
            pltpu.make_async_remote_copy(
                src_ref=ref, dst_ref=ref, send_sem=mod_send.at[p, a], recv_sem=mod_recv.at[source, a],
                device_id=(group, peer), device_id_type=MESH)
            for a, ref in enumerate(refs)
        ]

    sends = []
    for p, peer in enumerate(peers):
        sends += mod_copy(p, peer, me)
    for a, send in enumerate(sends):
        if a % 3 < 2:
            send.start()

    def dot(a, b):
        return lax.dot_general(a, b, (((1,), (0,)), ((), ())), precision=lax.Precision.DEFAULT, preferred_element_type=F32)

    def modulation(device):
        gain[steps_of(device), :] = 0.5 + 0.5 * gamma_raw[device].astype(F32)
        shift[steps_of(device), :] = 0.5 * beta_raw[device].astype(F32)

    def gelu(pre_act, a, b):
        half = pre_act * a + b
        u = half * ((8 * GELU_C * 0.044715) * (half * half) + 2 * GELU_C)
        return half * jnp.tanh(u) + half

    def activate(source, n, count, rows, mod, shared=False):
        cols = slice(n * TILE, (n + 1) * TILE)
        for k in range(count):
            a, b = mod(k, cols)
            for r in range(0, rows, STRIP):
                q = r if shared else k * rows + r
                act[k * rows + r:k * rows + r + STRIP, cols] = gelu(source[q:q + STRIP, cols], a, b)

    def mod_rows(steps):
        def rows(k, cols):
            row = span(steps[k], 1)
            return jnp.broadcast_to(gain[row, cols], (STRIP, TILE)), jnp.broadcast_to(shift[row, cols], (STRIP, TILE))
        return rows

    for load in loads[2:-1]:
        load.wait()
    modulation(me)
    for k in range(OWN):
        h_rows[pl.ds(me * OWN + k, 1), :] = jnp.broadcast_to(h_own[:, k:k + 1], (1, 128))
    x_own = latent[FIRST[1] - 1]
    for n in range(TILES):
        hidden0[:, n * TILE:(n + 1) * TILE] = dot(x_own, w_in[n])

    def steps0(device):
        return mod_rows([device * OWN + k for k in range(OWN)])

    def project0(device):
        half = OWN * ROWS // 2
        for i in range(2):
            rows = pl.ds(pl.multiple_of(device * (OWN * ROWS) + i * half, half), half)
            drift0[rows] = dot(act[i * half:(i + 1) * half, :], w_out[...])

    def chain0(first, last):
        for r in range(0, ROWS, 64):
            for c in range(0, C, 128):
                total = latent[FIRST[1] - 1 + first, r:r + 64, c:c + 128]
                for j in range(first, last):
                    h = jnp.broadcast_to(h_rows[j:j + 1, :], (64, 128))
                    total = total + drift0[j * ROWS + r:j * ROWS + r + 64, c:c + 128] * h
                    latent[FIRST[1] + j, r:r + 64, c:c + 128] = total

    other = 2 - 2 * (me // 2)

    def ordered(k):
        if isinstance(k, int):
            return (me, near, other, other + 1)[k]
        return jnp.where(k == 0, me, jnp.where(k == 1, near, other + k - 2))

    for n in range(TILES):
        activate(hidden0, n, OWN, ROWS, steps0(me), True)
    for send in sends[2::3]:
        send.start()
    loads[-1].wait()

    def loop0(k, carry):
        for copy in mod_copy(0, near, ordered(k))[:2]:
            copy.wait_recv()
        modulation(ordered(k))
        project0(ordered(k - 1))
        for n in range(TILES):
            activate(hidden0, n, OWN, ROWS, steps0(ordered(k)), True)
        return carry

    lax.fori_loop(1, 4, loop0, 0)
    for k in range(1, 4):
        mod_copy(0, near, ordered(k))[2].wait_recv()

    def chunk(t):
        return FIRST[1] + t * UNITS

    def unit_mods(base):
        return mod_rows([step_of(base + k) for k in range(UNITS)])

    def project_in(base, n):
        rows = latent[span(base, UNITS)].reshape(BATCH, C)
        pre[:, n * TILE:(n + 1) * TILE] = dot(rows, w_in[n])

    def project_out(count, parts=1):
        rows = count // parts
        return [dot(act[i * rows:(i + 1) * rows, :], w_out[...]) for i in range(parts)]

    def keep(drifts):
        first = 0
        for part in drifts:
            drift[first:first + part.shape[0]] = part
            first += part.shape[0]

    def accumulate(base, drifts=None):
        for k in range(UNITS):
            unit = base + k
            h = h_rows[span(step_of(unit), 1), :]
            h = jnp.broadcast_to(jnp.concatenate([h, h], axis=1), (ROWS, C))
            ahead = sweep_values(unit, (31, 30, 30))
            if isinstance(unit, int):
                start = unit if unit in FIRST else unit + ahead - 1
            else:
                start = jnp.where((unit == FIRST[1]) | (unit == FIRST[2]) | (unit == FIRST[3]), unit, unit + ahead - 1)
            latent[unit + ahead] = latent[start] + (drift if drifts is None else drifts)[k * ROWS:(k + 1) * ROWS] * h

    def steps(*bodies):
        def turn(i, carry):
            for k, body in enumerate(bodies):
                pl.when(i == k)(body)
            return carry

        lax.fori_loop(0, len(bodies), turn, 0)

    chain0(0, OWN)

    def first_chunk():
        for n in range(TILES):
            project_in(chunk(0), n)
        project0(ordered(3))
        for n in range(TILES):
            activate(pre, n, UNITS, ROWS, unit_mods(chunk(0)))

    def second_chunk():
        chain0(OWN, 2 * OWN)
        for n in range(TILES - 1):
            project_in(chunk(1), n)
        chain0(2 * OWN, STEPS)

    steps(first_chunk, second_chunk)

    def loop(t, carry):
        base = chunk(t)
        project_in(base + UNITS, TILES - 1)
        drifts = project_out(BATCH)
        for n in range(TILES):
            activate(pre, n, UNITS, ROWS, unit_mods(base + UNITS))
            if n < TILES - 1:
                project_in(base + 2 * UNITS, n)
        accumulate(base, drifts[0])
        return carry

    lax.fori_loop(0, CHUNKS - 2, loop, 0)

    tail = mod_rows(list(range(STEPS - TAIL, STEPS)))

    def section_in(q, n):
        rows = latent[FIRST[4] - TAIL:FIRST[4], q * SECTION:(q + 1) * SECTION].reshape(TAIL_BATCH, C)
        pre[0:TAIL_BATCH, n * TILE:(n + 1) * TILE] = dot(rows, w_in[n])

    def finish(q):
        for c in range(0, C, 128):
            total = latent[FIRST[4] - TAIL - 1 + 30, q * SECTION:(q + 1) * SECTION, c:c + 128]
            for k in range(TAIL):
                h = jnp.broadcast_to(h_rows[STEPS - TAIL + k:STEPS - TAIL + k + 1, :], (SECTION, 128))
                total = total + drift[k * SECTION:(k + 1) * SECTION, c:c + 128] * h
            y[rows_of(me, q * SECTION, SECTION), c:c + 128] = total

    def section_copy(q, source, target, send, recv):
        ref = y.at[rows_of(source, q * SECTION, SECTION)]
        return pltpu.make_async_remote_copy(
            src_ref=ref, dst_ref=ref, send_sem=send.at[q], recv_sem=recv.at[q], device_id=(group, target), device_id_type=MESH)

    def section_copies(q):
        copies = [section_copy(q, me, far, far_send, far_recv), section_copy(q, me, near, near_send, near_recv)]
        if q == SECTIONS - 1:
            copies.append(section_copy(q, me, diag, pass_send, pass_recv))
        return copies

    def send_section(q):
        for copy in section_copies(q):
            copy.start()

    def into(t, n):
        if t < CHUNKS:
            project_in(chunk(t), n)
        elif t < CHUNKS + SECTIONS:
            section_in(t - CHUNKS, n)

    def through(t, n):
        if t < CHUNKS:
            activate(pre, n, UNITS, ROWS, unit_mods(chunk(t)))
        elif t < CHUNKS + SECTIONS:
            activate(pre, n, TAIL, SECTION, tail)

    def tail_step(t):
        def body():
            into(t + 1, TILES - 1)
            drifts = project_out(BATCH if t < CHUNKS else TAIL_BATCH, 2 if EARLY and t == CHUNKS - 2 else 1)
            if EARLY and t == CHUNKS - 2:
                keep(drifts)
                accumulate(chunk(t))
            for n in range(TILES):
                through(t + 1, n)
                if n < TILES - 1:
                    into(t + 2, n)
            if not (EARLY and t == CHUNKS - 2):
                keep(drifts)
                if t < CHUNKS:
                    accumulate(chunk(t))
            if t >= CHUNKS:
                finish(t - CHUNKS)
                send_section(t - CHUNKS)
        return body

    def before_last():
        into(CHUNKS + SECTIONS - 1, TILES - 1)
        drifts = project_out(TAIL_BATCH, 2)
        for n in range(2):
            through(CHUNKS + SECTIONS - 1, n)
        keep(drifts)
        finish(SECTIONS - 2)
        send_section(SECTIONS - 2)

    def last():
        for n in range(2, TILES):
            through(CHUNKS + SECTIONS - 1, n)
        keep(project_out(TAIL_BATCH, 2))
        finish(SECTIONS - 1)

    steps(tail_step(CHUNKS - 2), tail_step(CHUNKS - 1))
    steps(tail_step(CHUNKS), tail_step(CHUNKS + 1))
    steps(before_last, last)
    send_section(SECTIONS - 1)

    own_copies = [section_copies(q) for q in range(SECTIONS)]
    pass_copies = [section_copy(q, far, near, pass_send, pass_recv) for q in range(SECTIONS - 1)]
    for q, copies in enumerate(own_copies):
        copies[0].wait_recv()
        if q < SECTIONS - 1:
            pass_copies[q].start()
    for q, copies in enumerate(own_copies):
        copies[1].wait_recv()
        (pass_copies[q] if q < SECTIONS - 1 else copies[2]).wait_recv()
    for copy in sends + [copy for copies in own_copies for copy in copies] + pass_copies:
        copy.wait_send()


def solution(mesh):
    vmem = pltpu.VMEM
    dma = pltpu.SemaphoreType.DMA
    sections = dma((SECTIONS,))
    def local_run(x_init, w_in, w_out, mod_gamma, mod_beta, step_size):
        hbm = pl.BlockSpec(memory_space=pl.ANY)
        out = pl.pallas_call(
            kernel,
            out_shape=vmem((4 * ROWS, C), F32),
            in_specs=[hbm] * 6,
            out_specs=pl.BlockSpec(memory_space=vmem),
            scratch_shapes=[
                vmem((TILES, C, TILE), BF16), vmem((H, C), BF16),
                vmem((4, OWN, H), BF16), vmem((4, OWN, H), BF16), vmem((1, OWN), F32), vmem((STEPS, 128), F32),
                vmem((STEPS, H), F32), vmem((STEPS, H), F32),
                vmem((ROWS, H), F32), vmem((BATCH, H), F32), vmem((OWN * ROWS, H), F32),
                vmem((FIRST[4] + 32, ROWS, C), F32), vmem((BATCH, C), F32), vmem((STEPS * ROWS, C), F32),
                dma((5 + TILES,)), dma((3, 3)), dma((4, 3)),
                sections, sections, sections, sections, sections, sections,
            ],
            compiler_params=pltpu.CompilerParams(collective_id=0, has_side_effects=True, vmem_limit_bytes=60 * 2 ** 20),
            name="picard",
        )(step_size.reshape(1, OWN), x_init.reshape(4 * ROWS, C), w_in, w_out, mod_gamma, mod_beta)
        return out.reshape(x_init.shape)

    return jax.shard_map(local_run, mesh=mesh, in_specs=(P("data", None, None), P(None, None), P(None, None), P("time", None), P("time", None), P("time")), out_specs=P("data", None, None), check_vma=False)
```

```python
import jax
import jax.numpy as jnp
from jax import lax
from jax.experimental import pallas as pl
from jax.experimental.pallas import tpu as pltpu
from jax.sharding import PartitionSpec as P

STEPS = 32
OWN = 8
ROWS = 128
C = 256
H = 1024
TILE = 256
TILES = H // TILE
FIRST = [0, 32, 63, 93, 122]
UNITS = 6
TAIL = 18
SECTION = 32
SECTIONS = ROWS // SECTION
CHUNKS = (FIRST[4] - TAIL - FIRST[1]) // UNITS
BATCH = UNITS * ROWS
TAIL_BATCH = TAIL * SECTION
EARLY = (FIRST[3] - 2 - FIRST[1]) // UNITS >= CHUNKS - 2
STRIP = 16
GELU_C = 0.7978845608028654
F32 = jnp.float32
BF16 = jnp.bfloat16
MESH = pl.DeviceIdType.MESH


def span(first, count):
    return slice(first, first + count) if isinstance(first, int) else pl.ds(first, count)


def sweep_values(unit, values):
    if isinstance(unit, int):
        return values[0] if unit < FIRST[2] else values[1] if unit < FIRST[3] else values[2]
    return jnp.where(unit < FIRST[2], values[0], jnp.where(unit < FIRST[3], values[1], values[2]))


def step_of(unit):
    return unit - sweep_values(unit, (FIRST[1] - 1, FIRST[2] - 2, FIRST[3] - 3))


def kernel(h_hbm, x_hbm, w_in_hbm, w_out_hbm, gamma_hbm, beta_hbm, y,
           w_in, w_out, gamma_raw, beta_raw, h_own, h_rows, gain, shift, hidden0, pre, act, latent, drift, drift0,
           load_sem, mod_send, mod_recv, near_send, near_recv, far_send, far_recv, pass_send, pass_recv):
    me = lax.axis_index("time")
    group = lax.axis_index("data")
    core = lax.rem(me, 2)
    near = me + 1 - 2 * core
    far = lax.rem(me + 2, 4)
    diag = lax.rem(near + 2, 4)
    peers = (near, far, diag)

    def rows_of(device, first=0, count=ROWS):
        return pl.ds(pl.multiple_of(device * ROWS + first, 8), count)

    def steps_of(device):
        return pl.ds(pl.multiple_of(device * OWN, OWN), OWN)

    loads = [
        pltpu.make_async_copy(gamma_hbm, gamma_raw.at[me], load_sem.at[0]),
        pltpu.make_async_copy(beta_hbm, beta_raw.at[me], load_sem.at[1]),
        pltpu.make_async_copy(h_hbm, h_own, load_sem.at[2]),
        pltpu.make_async_copy(x_hbm.at[rows_of(me)], latent.at[FIRST[1] - 1], load_sem.at[3]),
    ]
    for n in range(TILES):
        loads.append(pltpu.make_async_copy(w_in_hbm.at[:, pl.ds(n * TILE, TILE)], w_in.at[n], load_sem.at[4 + n]))
    loads.append(pltpu.make_async_copy(w_out_hbm, w_out, load_sem.at[4 + TILES]))
    for load in loads:
        load.start()

    barrier = pltpu.get_barrier_semaphore()
    for peer in peers:
        pl.semaphore_signal(barrier, inc=1, device_id=(group, peer), device_id_type=MESH)
    for load in loads[:2]:
        load.wait()
    pl.semaphore_wait(barrier, 3)

    def mod_copy(p, peer, source):
        refs = (gamma_raw.at[source], beta_raw.at[source], h_rows.at[steps_of(source)])
        return [
            pltpu.make_async_remote_copy(
                src_ref=ref, dst_ref=ref, send_sem=mod_send.at[p, a], recv_sem=mod_recv.at[source, a],
                device_id=(group, peer), device_id_type=MESH)
            for a, ref in enumerate(refs)
        ]

    sends = []
    for p, peer in enumerate(peers):
        sends += mod_copy(p, peer, me)
    for a, send in enumerate(sends):
        if a % 3 < 2:
            send.start()

    def dot(a, b):
        return lax.dot_general(a, b, (((1,), (0,)), ((), ())), precision=lax.Precision.DEFAULT, preferred_element_type=F32)

    def modulation(device):
        gain[steps_of(device), :] = 0.5 + 0.5 * gamma_raw[device].astype(F32)
        shift[steps_of(device), :] = 0.5 * beta_raw[device].astype(F32)

    def gelu(pre_act, a, b):
        half = pre_act * a + b
        u = half * ((8 * GELU_C * 0.044715) * (half * half) + 2 * GELU_C)
        return half * jnp.tanh(u) + half

    def activate(source, n, count, rows, mod, shared=False):
        cols = slice(n * TILE, (n + 1) * TILE)
        for k in range(count):
            a, b = mod(k, cols)
            for r in range(0, rows, STRIP):
                q = r if shared else k * rows + r
                act[k * rows + r:k * rows + r + STRIP, cols] = gelu(source[q:q + STRIP, cols], a, b)

    def mod_rows(steps):
        def rows(k, cols):
            row = span(steps[k], 1)
            return jnp.broadcast_to(gain[row, cols], (STRIP, TILE)), jnp.broadcast_to(shift[row, cols], (STRIP, TILE))
        return rows

    for load in loads[2:-1]:
        load.wait()
    modulation(me)
    for k in range(OWN):
        h_rows[pl.ds(me * OWN + k, 1), :] = jnp.broadcast_to(h_own[:, k:k + 1], (1, 128))
    x_own = latent[FIRST[1] - 1]
    for n in range(TILES):
        hidden0[:, n * TILE:(n + 1) * TILE] = dot(x_own, w_in[n])

    def steps0(device):
        return mod_rows([device * OWN + k for k in range(OWN)])

    def project0(device):
        half = OWN * ROWS // 2
        for i in range(2):
            rows = pl.ds(pl.multiple_of(device * (OWN * ROWS) + i * half, half), half)
            drift0[rows] = dot(act[i * half:(i + 1) * half, :], w_out[...])

    def chain0(first, last):
        for r in range(0, ROWS, 64):
            for c in range(0, C, 128):
                total = latent[FIRST[1] - 1 + first, r:r + 64, c:c + 128]
                for j in range(first, last):
                    h = jnp.broadcast_to(h_rows[j:j + 1, :], (64, 128))
                    total = total + drift0[j * ROWS + r:j * ROWS + r + 64, c:c + 128] * h
                    latent[FIRST[1] + j, r:r + 64, c:c + 128] = total

    other = 2 - 2 * (me // 2)

    def ordered(k):
        if isinstance(k, int):
            return (me, near, other, other + 1)[k]
        return jnp.where(k == 0, me, jnp.where(k == 1, near, other + k - 2))

    for n in range(TILES):
        activate(hidden0, n, OWN, ROWS, steps0(me), True)
    for send in sends[2::3]:
        send.start()
    loads[-1].wait()

    def loop0(k, carry):
        for copy in mod_copy(0, near, ordered(k))[:2]:
            copy.wait_recv()
        modulation(ordered(k))
        project0(ordered(k - 1))
        for n in range(TILES):
            activate(hidden0, n, OWN, ROWS, steps0(ordered(k)), True)
        return carry

    lax.fori_loop(1, 4, loop0, 0)
    for k in range(1, 4):
        mod_copy(0, near, ordered(k))[2].wait_recv()

    def chunk(t):
        return FIRST[1] + t * UNITS

    def unit_mods(base):
        return mod_rows([step_of(base + k) for k in range(UNITS)])

    def project_in(base, n):
        rows = latent[span(base, UNITS)].reshape(BATCH, C)
        pre[:, n * TILE:(n + 1) * TILE] = dot(rows, w_in[n])

    def project_out(count, parts=1):
        rows = count // parts
        return [dot(act[i * rows:(i + 1) * rows, :], w_out[...]) for i in range(parts)]

    def keep(drifts):
        first = 0
        for part in drifts:
            drift[first:first + part.shape[0]] = part
            first += part.shape[0]

    def accumulate(base, drifts=None):
        for k in range(UNITS):
            unit = base + k
            h = h_rows[span(step_of(unit), 1), :]
            h = jnp.broadcast_to(jnp.concatenate([h, h], axis=1), (ROWS, C))
            ahead = sweep_values(unit, (31, 30, 30))
            if isinstance(unit, int):
                start = unit if unit in FIRST else unit + ahead - 1
            else:
                start = jnp.where((unit == FIRST[1]) | (unit == FIRST[2]) | (unit == FIRST[3]), unit, unit + ahead - 1)
            latent[unit + ahead] = latent[start] + (drift if drifts is None else drifts)[k * ROWS:(k + 1) * ROWS] * h

    def steps(*bodies):
        def turn(i, carry):
            for k, body in enumerate(bodies):
                pl.when(i == k)(body)
            return carry

        lax.fori_loop(0, len(bodies), turn, 0)

    chain0(0, OWN)

    def first_chunk():
        for n in range(TILES):
            project_in(chunk(0), n)
        project0(ordered(3))
        for n in range(TILES):
            activate(pre, n, UNITS, ROWS, unit_mods(chunk(0)))

    def second_chunk():
        chain0(OWN, 2 * OWN)
        for n in range(TILES - 1):
            project_in(chunk(1), n)
        chain0(2 * OWN, STEPS)

    steps(first_chunk, second_chunk)

    def loop(t, carry):
        base = chunk(t)
        project_in(base + UNITS, TILES - 1)
        drifts = project_out(BATCH)
        for n in range(TILES):
            activate(pre, n, UNITS, ROWS, unit_mods(base + UNITS))
            if n < TILES - 1:
                project_in(base + 2 * UNITS, n)
        accumulate(base, drifts[0])
        return carry

    lax.fori_loop(0, CHUNKS - 2, loop, 0)

    tail = mod_rows(list(range(STEPS - TAIL, STEPS)))

    def section_in(q, n):
        rows = latent[FIRST[4] - TAIL:FIRST[4], q * SECTION:(q + 1) * SECTION].reshape(TAIL_BATCH, C)
        pre[0:TAIL_BATCH, n * TILE:(n + 1) * TILE] = dot(rows, w_in[n])

    def finish(q):
        for c in range(0, C, 128):
            total = latent[FIRST[4] - TAIL - 1 + 30, q * SECTION:(q + 1) * SECTION, c:c + 128]
            for k in range(TAIL):
                h = jnp.broadcast_to(h_rows[STEPS - TAIL + k:STEPS - TAIL + k + 1, :], (SECTION, 128))
                total = total + drift[k * SECTION:(k + 1) * SECTION, c:c + 128] * h
            y[rows_of(me, q * SECTION, SECTION), c:c + 128] = total

    def section_copy(q, source, target, send, recv):
        ref = y.at[rows_of(source, q * SECTION, SECTION)]
        return pltpu.make_async_remote_copy(
            src_ref=ref, dst_ref=ref, send_sem=send.at[q], recv_sem=recv.at[q], device_id=(group, target), device_id_type=MESH)

    def section_copies(q):
        copies = [section_copy(q, me, far, far_send, far_recv), section_copy(q, me, near, near_send, near_recv)]
        if q == SECTIONS - 1:
            copies.append(section_copy(q, me, diag, pass_send, pass_recv))
        return copies

    def send_section(q):
        for copy in section_copies(q):
            copy.start()

    def into(t, n):
        if t < CHUNKS:
            project_in(chunk(t), n)
        elif t < CHUNKS + SECTIONS:
            section_in(t - CHUNKS, n)

    def through(t, n):
        if t < CHUNKS:
            activate(pre, n, UNITS, ROWS, unit_mods(chunk(t)))
        elif t < CHUNKS + SECTIONS:
            activate(pre, n, TAIL, SECTION, tail)

    def tail_step(t):
        def body():
            into(t + 1, TILES - 1)
            drifts = project_out(BATCH if t < CHUNKS else TAIL_BATCH, 2 if EARLY and t == CHUNKS - 2 else 1)
            if EARLY and t == CHUNKS - 2:
                keep(drifts)
                accumulate(chunk(t))
            for n in range(TILES):
                through(t + 1, n)
                if n < TILES - 1:
                    into(t + 2, n)
            if not (EARLY and t == CHUNKS - 2):
                keep(drifts)
                if t < CHUNKS:
                    accumulate(chunk(t))
            if t >= CHUNKS:
                finish(t - CHUNKS)
                send_section(t - CHUNKS)
        return body

    def before_last():
        into(CHUNKS + SECTIONS - 1, TILES - 1)
        drifts = project_out(TAIL_BATCH, 2)
        for n in range(3):
            through(CHUNKS + SECTIONS - 1, n)
        keep(drifts)
        finish(SECTIONS - 2)
        send_section(SECTIONS - 2)

    def last():
        for n in range(3, TILES):
            through(CHUNKS + SECTIONS - 1, n)
        keep(project_out(TAIL_BATCH, 2))
        finish(SECTIONS - 1)

    steps(tail_step(CHUNKS - 2), tail_step(CHUNKS - 1))
    steps(tail_step(CHUNKS), tail_step(CHUNKS + 1))
    steps(before_last, last)
    send_section(SECTIONS - 1)

    own_copies = [section_copies(q) for q in range(SECTIONS)]
    pass_copies = [section_copy(q, far, near, pass_send, pass_recv) for q in range(SECTIONS - 1)]
    for q, copies in enumerate(own_copies):
        copies[0].wait_recv()
        if q < SECTIONS - 1:
            pass_copies[q].start()
    for q, copies in enumerate(own_copies):
        copies[1].wait_recv()
        (pass_copies[q] if q < SECTIONS - 1 else copies[2]).wait_recv()
    for copy in sends + [copy for copies in own_copies for copy in copies] + pass_copies:
        copy.wait_send()


def solution(mesh):
    vmem = pltpu.VMEM
    dma = pltpu.SemaphoreType.DMA
    sections = dma((SECTIONS,))
    def local_run(x_init, w_in, w_out, mod_gamma, mod_beta, step_size):
        hbm = pl.BlockSpec(memory_space=pl.ANY)
        out = pl.pallas_call(
            kernel,
            out_shape=vmem((4 * ROWS, C), F32),
            in_specs=[hbm] * 6,
            out_specs=pl.BlockSpec(memory_space=vmem),
            scratch_shapes=[
                vmem((TILES, C, TILE), BF16), vmem((H, C), BF16),
                vmem((4, OWN, H), BF16), vmem((4, OWN, H), BF16), vmem((1, OWN), F32), vmem((STEPS, 128), F32),
                vmem((STEPS, H), F32), vmem((STEPS, H), F32),
                vmem((ROWS, H), F32), vmem((BATCH, H), F32), vmem((OWN * ROWS, H), F32),
                vmem((FIRST[4] + 32, ROWS, C), F32), vmem((BATCH, C), F32), vmem((STEPS * ROWS, C), F32),
                dma((5 + TILES,)), dma((3, 3)), dma((4, 3)),
                sections, sections, sections, sections, sections, sections,
            ],
            compiler_params=pltpu.CompilerParams(collective_id=0, has_side_effects=True, vmem_limit_bytes=60 * 2 ** 20),
            name="picard",
        )(step_size.reshape(1, OWN), x_init.reshape(4 * ROWS, C), w_in, w_out, mod_gamma, mod_beta)
        return out.reshape(x_init.shape)

    return jax.shard_map(local_run, mesh=mesh, in_specs=(P("data", None, None), P(None, None), P(None, None), P("time", None), P("time", None), P("time")), out_specs=P("data", None, None), check_vma=False)
```
